32 devices in a mesh: row: 8 (over z, y), col: 4 (over x, core).
Axes of the slice: x: 2, y: 2, z: 4, core: 2. Of those that a mesh axis runs over, the one named last changes fastest.
Arguments:
- matrix: bfloat16 [32768, 32768], P('row', 'col'), may hold values from -0.03125 to 0.03125
- right_sides: float32 [32768, 64], P(('row', 'col')), may hold values from -6 to 6
- initial_guess: float32 [32768, 64], P(('row', 'col')), may hold values from -6 to 6
Outputs:
- solution: float32 [32768, 64], P(('row', 'col'))
The draws below stay inside these ranges and needn't reach their ends.
All inputs are finite; a program needn't handle non-finite values.
Results may differ from the reference program's by a relative error of at most 0.0038.
Values may be sent and summed in bfloat16 or wider, within the bound.
A program may use at most 128 MiB of HBM per device.

```python
import jax
import jax.numpy as jnp
from jax import lax

N = 32768
S = 64
STEPS = 3
PROW = 8
PCOL = 4
CH = 1024


def steps_of(stream_key, extent, cuts, least, high):
    factor_of, own = 1.0, jax.random.fold_in(stream_key, 6)
    for axis_at, parts in cuts:
        heights = jnp.exp(jax.random.uniform(jax.random.fold_in(own, axis_at), (parts,), jnp.float32, least / len(cuts), high / len(cuts)))
        factor_of = factor_of * jnp.repeat(heights, extent[axis_at] // parts).reshape([-1 if axis == axis_at else 1 for axis in range(len(extent))])
    return factor_of


def scatter_about(key, extent, scale, most, cuts=(), kind=jnp.bfloat16):
    factor_of = steps_of(key, extent, cuts, -0.22, 0.18) if cuts else 1.0
    values = jax.random.normal(key, extent, jnp.float32) * scale * factor_of
    return jnp.minimum(jnp.maximum(values, -most), most).astype(kind)


def setup_inputs(seed: int = 0) -> dict:
    splits = jax.random.split(jax.random.key(seed), 4)
    return {
        "matrix": scatter_about(splits[0], (N, N), N ** -0.5, 0.03125, ((0, 8), (1, 4))),
        "right_sides": scatter_about(splits[1], (N, S), 1.0, 6.0, ((0, 32),), jnp.float32),
        "initial_guess": scatter_about(splits[2], (N, S), 1.0, 6.0, ((0, 32),), jnp.float32),
    }


DIAGONAL_SHIFT = 1.4

def inner_products(left, right):
    return jnp.einsum('rk,rs->ks', left, right, precision=lax.Precision.HIGHEST)

def combine_basis(stacked, weights):
    return jnp.dot(stacked, weights, precision=lax.Precision.HIGHEST)

def orthonormal(applied, gram_sum):
    lower_factor = jnp.linalg.cholesky(gram_sum)
    basis_next = lax.linalg.triangular_solve(lower_factor, applied, left_side=False, lower=True, transpose_a=True)
    return (basis_next, lower_factor.T)

def least_squares(column_list, top_factor):
    span_width = top_factor.shape[0]
    count = len(column_list)
    pieces = []
    for position, (projected, upper_factor) in enumerate(column_list):
        filler = jnp.zeros(((count - position - 1) * span_width, span_width), jnp.float32)
        pieces.append(jnp.concatenate([projected, upper_factor, filler], axis=0))
    hessenberg = jnp.concatenate(pieces, axis=1)
    normal_matrix = inner_products(hessenberg, hessenberg)
    target = inner_products(hessenberg[:span_width], top_factor)
    lower_factor = jnp.linalg.cholesky(normal_matrix)
    halfway = lax.linalg.triangular_solve(lower_factor, target, left_side=True, lower=True)
    return lax.linalg.triangular_solve(lower_factor, halfway, left_side=True, lower=True, transpose_a=True)

def operate(block_now, matrix):
    rounded = lax.optimization_barrier(block_now.astype(jnp.bfloat16))
    ordered = rounded.reshape(PROW, PCOL, CH, S).transpose(1, 0, 2, 3).reshape(N, S).astype(jnp.float32)

    def row_panel(panel_rows):
        return jnp.dot(panel_rows.astype(jnp.float32), ordered, precision=lax.Precision.HIGHEST)
    product = lax.map(row_panel, matrix.reshape(PROW, N // PROW, N)).reshape(N, S)
    return DIAGONAL_SHIFT * block_now + product

def reference(matrix, right_sides, initial_guess):
    residual_start = right_sides - operate(initial_guess, matrix)
    basis_now, top_factor = orthonormal(residual_start, inner_products(residual_start, residual_start))
    basis_list = [basis_now]
    column_list = []
    for iteration in range(STEPS):
        applied = operate(basis_list[-1], matrix)
        stacked = jnp.concatenate(basis_list, axis=1)
        projected = inner_products(stacked, applied)
        applied = applied - combine_basis(stacked, projected)
        gram_sum = inner_products(applied, applied)
        basis_now, upper_factor = orthonormal(applied, gram_sum)
        basis_list.append(basis_now)
        column_list.append((projected, upper_factor))
    coefficients = least_squares(column_list, top_factor)
    update = combine_basis(jnp.concatenate(basis_list[:-1], axis=1), coefficients)
    return initial_guess + update
```

```python
import functools

import jax
import jax.numpy as jnp
from jax import lax
from jax.experimental import pallas as pl
from jax.experimental.pallas import tpu as pltpu
from jax.sharding import PartitionSpec as P

STEPS = 3
DIAGONAL_SHIFT = 1.4
MESH = pl.DeviceIdType.MESH
SLOT_BYTES = 40 * 1024 * 1024
VMEM = pl.BlockSpec(memory_space=pltpu.VMEM)


def bits_of(count):
    return [1 << b for b in range(count.bit_length() - 1)]


def flipped(me, weight):
    bit = lax.rem(lax.div(me, weight), 2)
    return me + weight * (1 - 2 * bit)


def dot_high(a, b, contract=(1, 0)):
    return lax.dot_general(
        a, b, (((contract[0],), (contract[1],)), ((), ())),
        precision=lax.Precision.HIGHEST, preferred_element_type=jnp.float32,
    )


def greet(peers):
    barrier = pltpu.get_barrier_semaphore()
    for peer in peers:
        pl.semaphore_signal(barrier, inc=1, device_id=peer, device_id_type=MESH)
    pl.semaphore_wait(barrier, len(peers))


def operate_kernel(rows, cols, slots, own_ref, matrix_ref, out_ref, tiles, gathered, acc, parts, landed,
                   tile_sem, zs, zr, ys, yr, rs, rr):
    row, col = lax.axis_index("row"), lax.axis_index("col")
    width, chunk = own_ref.shape
    panel = matrix_ref.shape[0]
    half = rows // 2
    a, b = lax.div(row, 2), lax.rem(row, 2)
    partner = (a * 2 + (1 - b), col)

    def source(d):
        return lax.rem(a - d + half, half) * 2

    plan = [(0, False), (0, True)]
    for d in range(1, half):
        plan += [(d, False), (d, True)]

    def block_index(step):
        d, other = plan[step]
        return source(d) + ((1 - b) if other else b)

    def fetch(step):
        columns = pl.ds(pl.multiple_of(block_index(step) * chunk, chunk), chunk)
        return pltpu.make_async_copy(
            matrix_ref.at[:, columns], tiles.at[step % slots], tile_sem.at[step % slots]
        )

    for step in range(slots):
        fetch(step).start()

    peers = [(lax.rem(a + d, half) * 2 + b, col) for d in range(1, half)]
    greet(peers + [partner] + [(row, flipped(col, w)) for w in bits_of(cols)])

    def to_partner(d):
        src = own_ref if d == 0 else gathered.at[source(d) + b]
        return pltpu.make_async_remote_copy(
            src_ref=src, dst_ref=gathered.at[source(d) + b],
            send_sem=ys.at[d], recv_sem=yr.at[d], device_id=partner, device_id_type=MESH,
        )

    def along(d):
        return pltpu.make_async_remote_copy(
            src_ref=own_ref, dst_ref=gathered.at[row],
            send_sem=zs.at[d], recv_sem=zr.at[d], device_id=peers[d - 1], device_id_type=MESH,
        )

    to_partner(0).start()
    for d in range(1, half):
        along(d).start()

    tile_rows = min(panel, 512)

    def multiply(step):
        d, other = plan[step]
        if other:
            to_partner(d).wait_recv()
        fetch(step).wait()
        block = own_ref[...] if step == 0 else gathered[block_index(step)]
        q = block.astype(jnp.float32).T.astype(jnp.bfloat16)
        slot = step % slots

        @pl.loop(0, panel // tile_rows)
        def _(i):
            at = pl.ds(pl.multiple_of(i * tile_rows, tile_rows), tile_rows)
            product = jnp.dot(tiles[slot, at, :], q, preferred_element_type=jnp.float32)
            if step == 0:
                acc[at, :] = product
            else:
                acc[at, :] += product

        if step + slots < rows:
            fetch(step + slots).start()

    arrived = 1
    for step in range(rows):
        if step >= 1 and arrived < half:
            along(arrived).wait_recv()
            to_partner(arrived).start()
            arrived += 1
        multiply(step)

    @pl.loop(0, cols)
    def _(c):
        parts[c] = acc[pl.ds(pl.multiple_of(c * chunk, chunk), chunk), :].T

    base = 0
    sends = []
    for w in bits_of(cols):
        low, bit = lax.rem(col, w), lax.rem(lax.div(col, w), 2)
        other_col = flipped(col, w)
        count = cols // (2 * w)
        copies = []
        for j in range(count):
            copies.append(pltpu.make_async_remote_copy(
                src_ref=parts.at[low + (1 - bit) * w + j * 2 * w], dst_ref=landed.at[base + j],
                send_sem=rs.at[base + j], recv_sem=rr.at[base + j],
                device_id=(row, other_col), device_id_type=MESH,
            ))
            copies[-1].start()
        for j in range(count):
            copies[j].wait_recv()
            mine = low + bit * w + j * 2 * w
            parts[mine] = parts[mine] + landed[base + j]
        sends += copies
        base += count
    out_ref[...] = parts[col]
    for copy in sends:
        copy.wait_send()
    for d in range(half):
        to_partner(d).wait_send()
    for d in range(1, half):
        along(d).wait_send()


def operate(own, matrix, rows, cols):
    width, chunk = own.shape
    panel = matrix.shape[0]
    slots = max(1, min(rows, SLOT_BYTES // (panel * chunk * 2)))
    half = rows // 2
    landings = max(1, cols - 1)
    dma = pltpu.SemaphoreType.DMA
    return pl.pallas_call(
        functools.partial(operate_kernel, rows, cols, slots),
        out_shape=jax.ShapeDtypeStruct((width, chunk), jnp.float32),
        in_specs=[VMEM, pl.BlockSpec(memory_space=pl.ANY)],
        out_specs=VMEM,
        scratch_shapes=[
            pltpu.VMEM((slots, panel, chunk), jnp.bfloat16),
            pltpu.VMEM((rows, width, chunk), jnp.bfloat16),
            pltpu.VMEM((panel, width), jnp.float32),
            pltpu.VMEM((cols, width, chunk), jnp.float32),
            pltpu.VMEM((landings, width, chunk), jnp.float32),
            dma((slots,)), dma((half,)), dma((half,)), dma((half,)), dma((half,)),
            dma((landings,)), dma((landings,)),
        ],
        compiler_params=pltpu.CompilerParams(
            collective_id=0, has_side_effects=True, vmem_limit_bytes=60 * 1024 * 1024
        ),
        name="operate",
    )(own, matrix)


def gram_kernel(rows, cols, left_ref, right_ref, out_ref, held, landed, send_sem, recv_sem):
    row, col = lax.axis_index("row"), lax.axis_index("col")
    partners = [(row, flipped(col, w)) for w in bits_of(cols)]
    partners += [(flipped(row, w), col) for w in bits_of(rows)]
    held[0] = dot_high(left_ref[...], right_ref[...], (1, 1))
    greet(partners)
    copies = []
    for i, partner in enumerate(partners):
        copy = pltpu.make_async_remote_copy(
            src_ref=held.at[i], dst_ref=landed.at[i], send_sem=send_sem.at[i],
            recv_sem=recv_sem.at[i], device_id=partner, device_id_type=MESH,
        )
        copy.start()
        copy.wait_recv()
        total = held[i] + landed[i]
        if i + 1 < len(partners):
            held[i + 1] = total
        else:
            out_ref[...] = total
        copies.append(copy)
    for copy in copies:
        copy.wait_send()


def gram_total(left, right, rows, cols, ident):
    shape = (left.shape[0], right.shape[0])
    n = len(bits_of(rows)) + len(bits_of(cols))
    return pl.pallas_call(
        functools.partial(gram_kernel, rows, cols),
        out_shape=jax.ShapeDtypeStruct(shape, jnp.float32),
        in_specs=[VMEM, VMEM],
        out_specs=VMEM,
        scratch_shapes=[
            pltpu.VMEM((n,) + shape, jnp.float32), pltpu.VMEM((n,) + shape, jnp.float32),
            pltpu.SemaphoreType.DMA((n,)), pltpu.SemaphoreType.DMA((n,)),
        ],
        compiler_params=pltpu.CompilerParams(collective_id=ident, has_side_effects=True),
        name=f"gram{ident}",
    )(left, right)


def factor(gram):
    n = gram.shape[0]
    i = lax.broadcasted_iota(jnp.int32, (n, n), 0)
    j = lax.broadcasted_iota(jnp.int32, (n, n), 1)
    work = jnp.concatenate([gram, (i == j).astype(jnp.float32)], axis=1)
    at_row = lax.broadcasted_iota(jnp.int32, work.shape, 0)
    scale = jnp.ones((n, 1), jnp.float32)
    at = lax.broadcasted_iota(jnp.int32, (n, 1), 0)
    for k in range(n):
        pivot = work[k:k + 1, k:k + 1]
        line = work[k:k + 1, :] * (1.0 / pivot)
        scale = jnp.where(at == k, pivot, scale)
        work = work - jnp.where(at_row > k, work[:, k:k + 1] * line, 0.0)
    work = work * (1.0 / jnp.sqrt(scale))
    upper = jnp.where(j >= i, work[:, :n], 0.0)
    inverse = jnp.where(j <= i, work[:, n:], 0.0)
    return upper, inverse


def first_kernel(gram_ref, block_ref, basis_ref, upper_ref):
    upper, inverse = factor(gram_ref[...])
    upper_ref[...] = upper
    basis_ref[...] = dot_high(inverse, block_ref[...])


def step_kernel(gram_ref, block_ref, stacked_ref, basis_ref, upper_ref):
    span = stacked_ref.shape[0]
    sums = gram_ref[...]
    projected = sums[:, :span]
    upper, inverse = factor(sums[:, span:] - dot_high(projected, projected, (1, 1)))
    upper_ref[...] = upper
    cleaned = block_ref[...] - dot_high(projected, stacked_ref[...])
    basis_ref[...] = dot_high(inverse, cleaned)


def orthonormal(kernel, width, chunk, *operands):
    return pl.pallas_call(
        kernel,
        out_shape=(
            jax.ShapeDtypeStruct((width, chunk), jnp.float32),
            jax.ShapeDtypeStruct((width, width), jnp.float32),
        ),
        in_specs=[VMEM] * len(operands),
        out_specs=(VMEM, VMEM),
        name="orthonormal",
    )(*operands)


def solve_kernel(count, normal_ref, target_ref, out_ref):
    w = target_ref.shape[1]

    def cut(k):
        return slice(k * w, (k + 1) * w)

    normal = {(p, q): normal_ref[cut(p), cut(q)] for p in range(count) for q in range(p, count)}
    halfway = [target_ref[cut(p), :] for p in range(count)]
    inverses, upper = [], {}
    for p in range(count):
        _, inverse = factor(normal[p, p])
        inverses.append(inverse)
        halfway[p] = dot_high(inverse, halfway[p])
        for q in range(p + 1, count):
            upper[p, q] = dot_high(inverse, normal[p, q])
        for q in range(p + 1, count):
            halfway[q] = halfway[q] - dot_high(upper[p, q], halfway[p], (0, 0))
            for s in range(q, count):
                normal[q, s] = normal[q, s] - dot_high(upper[p, q], upper[p, s], (0, 0))
    for p in reversed(range(count)):
        value = halfway[p]
        for q in range(p + 1, count):
            value = value - dot_high(upper[p, q], out_ref[cut(q), :])
        out_ref[cut(p), :] = dot_high(inverses[p], value, (0, 0))


def least_squares(column_list, top_factor):
    width = top_factor.shape[0]
    count = len(column_list)
    pieces = []
    for position, (projected, upper_factor) in enumerate(column_list):
        filler = jnp.zeros(((count - position - 1) * width, width), jnp.float32)
        pieces.append(jnp.concatenate([projected, upper_factor, filler], axis=0))
    hessenberg = jnp.concatenate(pieces, axis=1)
    normal = dot_high(hessenberg, hessenberg, (0, 0))
    target = dot_high(hessenberg[:width], top_factor, (0, 0))
    return pl.pallas_call(
        functools.partial(solve_kernel, count),
        out_shape=jax.ShapeDtypeStruct(target.shape, jnp.float32),
        in_specs=[VMEM, VMEM],
        out_specs=VMEM,
        name="least_squares",
    )(normal, target)


def per_device(rows, cols, matrix, right_sides, initial_guess):
    guess, sides = initial_guess.T, right_sides.T
    width, chunk = guess.shape

    def apply(block):
        return DIAGONAL_SHIFT * block + operate(block.astype(jnp.bfloat16), matrix, rows, cols)

    residual = sides - apply(guess)
    gram = gram_total(residual, residual, rows, cols, 1)
    basis, top_factor = orthonormal(first_kernel, width, chunk, gram, residual)
    basis_list, column_list = [basis], []
    for iteration in range(STEPS):
        applied = apply(basis_list[-1])
        stacked = jnp.concatenate(basis_list, axis=0)
        sums = gram_total(
            applied, jnp.concatenate([stacked, applied], axis=0), rows, cols, 2 + iteration
        )
        basis, upper = orthonormal(step_kernel, width, chunk, sums, applied, stacked)
        basis_list.append(basis)
        column_list.append((sums[:, : stacked.shape[0]].T, upper))
    coefficients = least_squares(column_list, top_factor)
    return initial_guess + dot_high(stacked, coefficients, (0, 0))


def solution(mesh):
    return jax.shard_map(
        functools.partial(per_device, mesh.shape["row"], mesh.shape["col"]),
        mesh=mesh,
        in_specs=(P("row", "col"), P(("row", "col"), None), P(("row", "col"), None)),
        out_specs=P(("row", "col"), None),
        check_vma=False,
    )
```
